32 devices in a mesh: dom: 4 (over z), col: 8 (over y, x, core).
Axes of the slice: x: 2, y: 2, z: 4, core: 2. Of those that a mesh axis runs over, the one named last changes fastest.
Arguments:
- rhs_interior: bfloat16 [4, 48, 8192], P('dom', 'col'), may hold values from -6 to 6
- interior_inv: bfloat16 [4, 8192, 8192], P('dom', None, 'col'), may hold values from -0.0625 to 0.0625
- coupling: bfloat16 [4, 8192, 768], P('dom', 'col'), may hold values from -0.0625 to 0.0625
- rhs_interface: bfloat16 [48, 8192], P('col', 'dom'), may hold values from -6 to 6
- block_ids: int32 [4, 6], P('dom'), may hold values from 0 to 63, as said below
- interface_inv: bfloat16 [8192, 8192], P('dom', 'col'), may hold values from -0.0625 to 0.0625
Outputs:
- interior_solution: bfloat16 [4, 48, 8192], P('dom', None, 'col')
- interface_solution: bfloat16 [48, 8192], P('col')
The draws below stay inside these ranges and needn't reach their ends.
Inputs may be any that keep to these rules, and one draw needn't show every extreme that they name: `block_ids`: each row names 6 different blocks.
All inputs are finite; a program needn't handle non-finite values.
Results may differ from the reference program's by a relative error of at most 0.025.
Values may be sent and summed in bfloat16 or wider, within the bound.
A program may use at most 64 MiB of HBM per device.

```python
import jax
import jax.numpy as jnp
from jax import lax

NI = 8192
G = 8192
BS = 128
KB = 6
NSUB = 4
R = 48
LI = 768


def draw_block_ids(key, part):
    keys = jax.random.split(jax.random.fold_in(key, 7), NSUB)
    orders = jax.vmap(lambda single: jax.random.permutation(single, G // BS))(keys)
    return orders[:, :KB].astype(jnp.int32)


def shard_levels(rng, shape, cuts, low, top_value):
    level = 1.0
    for dim, parts in cuts:
        draws = jax.random.uniform(jax.random.fold_in(jax.random.fold_in(rng, 6), dim), (parts,), jnp.float32, low / len(cuts), top_value / len(cuts))
        level = level * jnp.repeat(jnp.exp(draws), shape[dim] // parts).reshape((-1,) + (1,) * (len(shape) - 1 - dim))
    return level


def gaussian(rng, shape, scale, bound, shards=(), held_as=jnp.bfloat16):
    drawn = jax.random.normal(rng, shape, jnp.float32) * scale
    if len(shards) > 0:
        drawn = shard_levels(rng, shape, shards, -0.22, 0.18) * drawn
    return jnp.clip(drawn, min=-bound, max=bound).astype(held_as)


def setup_inputs(seed: int = 0) -> dict:
    arg_keys = jax.random.split(jax.random.key(seed), 7)
    rhs_interior = gaussian(arg_keys[0], (NSUB, R, NI), 1.0, 6.0, ((0, 4), (1, 8)))
    interior_inv = gaussian(arg_keys[1], (NSUB, NI, NI), NI ** -0.5, 0.0625, ((0, 4), (2, 8)))
    coupling = gaussian(arg_keys[2], (NSUB, NI, LI), NI ** -0.5, 0.0625, ((0, 4), (1, 8)))
    rhs_interface = gaussian(arg_keys[3], (R, G), 1.0, 6.0, ((0, 8), (1, 4)))
    block_ids = draw_block_ids(jax.random.fold_in(arg_keys[6], 71), 0)
    interface_inv = gaussian(arg_keys[5], (G, G), G ** -0.5, 0.0625, ((0, 4), (1, 8)))
    return {"rhs_interior": rhs_interior, "interior_inv": interior_inv, "coupling": coupling, "rhs_interface": rhs_interface, "block_ids": block_ids, "interface_inv": interface_inv}


def reference(rhs_interior, interior_inv, coupling, rhs_interface, block_ids, interface_inv):
    nblocks = G // BS
    onehot = (block_ids[:, :, None] == jnp.arange(nblocks, dtype=jnp.int32)[None, None, :]).astype(jnp.float32)

    def forward(running, items):
        rhs_block, inverse, couple, select = items
        step = jnp.dot(rhs_block, inverse, preferred_element_type=jnp.float32).astype(jnp.bfloat16)
        contribution = jnp.dot(step, couple, preferred_element_type=jnp.float32)
        placed = jnp.einsum("kb,rks->rbs", select, contribution.reshape(R, KB, BS)).reshape(R, G)
        return running + placed, None

    summed, unused = lax.scan(forward, jnp.zeros((R, G), jnp.float32), (rhs_interior, interior_inv, coupling, onehot))
    reduced = (rhs_interface.astype(jnp.float32) - summed).astype(jnp.bfloat16)
    interface_solution = jnp.dot(reduced, interface_inv, preferred_element_type=jnp.float32).astype(jnp.bfloat16)
    solution_blocks = interface_solution.astype(jnp.float32).reshape(R, nblocks, BS)

    def backward(items):
        rhs_block, inverse, couple, select = items
        local_solution = jnp.einsum("kb,rbs->rks", select, solution_blocks).reshape(R, LI).astype(jnp.bfloat16)
        correction = jnp.dot(local_solution, couple.T, preferred_element_type=jnp.float32)
        interior_rhs = (rhs_block.astype(jnp.float32) - correction).astype(jnp.bfloat16)
        return jnp.dot(interior_rhs, inverse, preferred_element_type=jnp.float32).astype(jnp.bfloat16)

    interior_solution = lax.map(backward, (rhs_interior, interior_inv, coupling, onehot))
    return interior_solution, interface_solution
```

```python
import functools

import jax
import jax.numpy as jnp
from jax import lax
from jax.experimental import pallas as pl
from jax.experimental.pallas import tpu as pltpu
from jax.sharding import PartitionSpec as P

BF = jnp.bfloat16
F32 = jnp.float32
MESH = pl.DeviceIdType.MESH
LANES = 128
CHUNKS = 4


def partner(me, o, n):
    total, bit = 0, 1
    while bit < n:
        total = total + lax.rem(lax.div(me, bit) + (o // bit) % 2, 2) * bit
        bit *= 2
    return total


def kernel(C, D, ids_ref, rhs_ref, ri_ref, inv_hbm, cp_hbm, ii_hbm, out_ref, sol_ref,
           inv, cp, ii, gath, xf, xg, xl, rhsl, idsb, s2, r2, g3, acc3, g4, s5, r5,
           s6, r6, g7, x8, r9, g10, stepb,
           ld, ss, rs, s1sem, r1sem):
    c = lax.axis_index("col")
    d = lax.axis_index("dom")
    rl, ni = rhs_ref.shape
    nl = inv.shape[1]
    li = cp.shape[1]
    gl = ii.shape[0]
    gc = ii.shape[1]
    kb = li // LANES
    w = ni // CHUNKS

    loads = []
    for j in range(CHUNKS):
        rows = pl.ds(j * w, w)
        loads.append(pltpu.make_async_copy(inv_hbm.at[rows, :], inv.at[rows, :], ld.at[j]))
    loads.append(pltpu.make_async_copy(cp_hbm, cp, ld.at[CHUNKS]))
    loads.append(pltpu.make_async_copy(ii_hbm, ii, ld.at[CHUNKS + 1]))
    for copy in loads:
        copy.start()

    barrier = pltpu.get_barrier_semaphore()
    for o in range(1, C):
        pl.semaphore_signal(barrier, inc=1, device_id={"col": partner(c, o, C)}, device_id_type=MESH)
    for o in range(1, D):
        pl.semaphore_signal(barrier, inc=1, device_id={"dom": partner(d, o, D)}, device_id_type=MESH)
    pl.semaphore_wait(barrier, C - 1 + D - 1)

    def send(src, dst, phase, o, axis, target):
        copy = pltpu.make_async_remote_copy(
            src_ref=src, dst_ref=dst, send_sem=ss.at[phase, o], recv_sem=rs.at[phase, o],
            device_id={axis: target}, device_id_type=MESH)
        copy.start()
        return copy

    done = []

    first = []
    for j in range(CHUNKS):
        cols = pl.ds(j * w, w)
        row = []
        for o in range(1, C):
            copy = pltpu.make_async_remote_copy(
                src_ref=rhs_ref.at[:, cols], dst_ref=gath.at[c, :, cols],
                send_sem=s1sem.at[j, o], recv_sem=r1sem.at[j, o],
                device_id={"col": partner(c, o, C)}, device_id_type=MESH)
            copy.start()
            row.append(copy)
        first.append(row)
        done += row
    gath[c] = rhs_ref[...]
    for k in range(kb):
        idsb[d, :, k * LANES:(k + 1) * LANES] = jnp.full((8, LANES), ids_ref[0, k], jnp.int32)
    idcopies = [send(idsb.at[d], idsb.at[d], 0, o, "dom", partner(d, o, D)) for o in range(1, D)]
    done += idcopies

    acc = None
    for j in range(CHUNKS):
        for copy in first[j]:
            copy.wait_recv()
        for q in range(C):
            xf[q * rl:(q + 1) * rl, :] = gath[q, :, j * w:(j + 1) * w].astype(F32)
        loads[j].wait()
        part = jnp.dot(xf[...].astype(BF), inv[j * w:(j + 1) * w, :], preferred_element_type=F32)
        acc = part if acc is None else acc + part
    stepb[...] = acc.astype(BF)

    loads[CHUNKS].wait()
    con = jnp.dot(stepb[...], cp[...], preferred_element_type=F32)
    for q in range(C):
        s2[q] = con[q * rl:(q + 1) * rl, :].astype(BF)
    copies = []
    for o in range(1, C):
        t = partner(c, o, C)
        copies.append(send(s2.at[t], r2.at[c], 1, o, "col", t))
    done += copies
    r2[c] = s2[c]
    for q in range(C):
        rhsl[q * rl:(q + 1) * rl, :] = gath[q, :, pl.ds(pl.multiple_of(c * nl, LANES), nl)].astype(F32)
    for copy in copies:
        copy.wait_recv()
    total = r2[0].astype(F32)
    for q in range(1, C):
        total = total + r2[q].astype(F32)

    g3[d] = total.astype(BF)
    copies = [send(g3.at[d], g3.at[d], 2, o, "dom", partner(d, o, D)) for o in range(1, D)]
    done += copies
    acc3[...] = ri_ref[...].astype(F32)
    for copy in idcopies:
        copy.wait_recv()
    for copy in copies:
        copy.wait_recv()
    base = d * (gl // LANES)

    def place(s, carry):
        ids = [idsb[s, 0:rl, k * LANES:(k + 1) * LANES] - base for k in range(kb)]
        val = [g3[s, :, k * LANES:(k + 1) * LANES].astype(F32) for k in range(kb)]
        for j in range(gl // LANES):
            part = jnp.zeros((rl, LANES), F32)
            for k in range(kb):
                part = jnp.where(ids[k] == j, val[k], part)
            at = slice(j * LANES, (j + 1) * LANES)
            acc3[:, at] = acc3[:, at] - part
        return carry

    lax.fori_loop(0, D, place, 0)

    g4[c] = acc3[...].astype(BF)
    copies = [send(g4.at[c], g4.at[c], 3, o, "col", partner(c, o, C)) for o in range(1, C)]
    done += copies
    loads[CHUNKS + 1].wait()
    for copy in copies:
        copy.wait_recv()
    for q in range(C):
        xg[q * rl:(q + 1) * rl, :] = g4[q].astype(F32)
    part = jnp.dot(xg[...].astype(BF), ii[...], preferred_element_type=F32)

    for q in range(C):
        s5[q] = part[q * rl:(q + 1) * rl, :].astype(BF)
    copies = []
    for o in range(1, C):
        t = partner(c, o, C)
        copies.append(send(s5.at[t], r5.at[c], 4, o, "col", t))
    done += copies
    r5[c] = s5[c]
    for copy in copies:
        copy.wait_recv()

    per = gc // LANES

    def pick(s, carry):
        ids = [idsb[s, 0:rl, k * LANES:(k + 1) * LANES] for k in range(kb)]
        got = [jnp.zeros((rl, LANES), F32) for k in range(kb)]
        for q in range(C):
            for j in range(per):
                block = r5[q, :, j * LANES:(j + 1) * LANES].astype(F32)
                got = [jnp.where(ids[k] == q * per + j, block, got[k]) for k in range(kb)]
        for k in range(kb):
            s6[s, :, k * LANES:(k + 1) * LANES] = got[k].astype(BF)
        return carry

    lax.fori_loop(0, D, pick, 0)
    copies = []
    for o in range(1, D):
        t = partner(d, o, D)
        copies.append(send(s6.at[t], r6.at[d], 5, o, "dom", t))
    done += copies
    span = C // D
    ninth = []
    for o in range(1, D):
        t = partner(d, o, D)
        ninth.append(send(r5.at[pl.ds(t * span, span)], r9.at[d], 6, o, "dom", t))
    done += ninth
    r6[d] = s6[d]
    for q in range(span):
        r9[d, q] = r5[d * span + q]
    for copy in copies:
        copy.wait_recv()
    total = r6[0].astype(F32)
    for s in range(1, D):
        total = total + r6[s].astype(F32)

    g7[c] = total.astype(BF)
    copies = [send(g7.at[c], g7.at[c], 7, o, "col", partner(c, o, C)) for o in range(1, C)]
    done += copies
    for copy in copies:
        copy.wait_recv()
    for q in range(C):
        xl[q * rl:(q + 1) * rl, :] = g7[q].astype(F32)
    corr = lax.dot_general(xl[...].astype(BF), cp[...], (((1,), (1,)), ((), ())), preferred_element_type=F32)

    x8[c] = (rhsl[...] - corr).astype(BF)
    copies = [send(x8.at[c], x8.at[c], 8, o, "col", partner(c, o, C)) for o in range(1, C)]
    done += copies

    for copy in ninth:
        copy.wait_recv()
    for q in range(span):
        total = r9[0, q].astype(F32)
        for s in range(1, D):
            total = total + r9[s, q].astype(F32)
        g10[d, q] = total.astype(BF)
    tenth = [send(g10.at[d], g10.at[d], 9, o, "dom", partner(d, o, D)) for o in range(1, D)]
    done += tenth

    acc = None
    for o in range(C):
        q = partner(c, o, C)
        if o > 0:
            copies[o - 1].wait_recv()
        part = jnp.dot(x8[q], inv[pl.ds(pl.multiple_of(q * nl, LANES), nl), :], preferred_element_type=F32)
        acc = part if acc is None else acc + part
    out_ref[...] = acc.astype(BF)

    for copy in tenth:
        copy.wait_recv()
    for s in range(D):
        for q in range(span):
            at = (s * span + q) * gc
            sol_ref[:, at:at + gc] = g10[s, q]
    for copy in done:
        copy.wait_send()


def per_device(C, D, rhs_interior, interior_inv, coupling, rhs_interface, block_ids, interface_inv):
    rl, ni = rhs_interior.shape[1:]
    nl = interior_inv.shape[2]
    li = coupling.shape[2]
    gl, gc = interface_inv.shape
    r = rl * C
    span = C // D
    vmem = pl.BlockSpec(memory_space=pltpu.VMEM)
    hbm = pl.BlockSpec(memory_space=pl.ANY)
    scratch = [
        pltpu.VMEM((ni, nl), BF), pltpu.VMEM((coupling.shape[1], li), BF), pltpu.VMEM((gl, gc), BF),
        pltpu.VMEM((C, rl, ni), BF),
        pltpu.VMEM((r, ni // CHUNKS), F32), pltpu.VMEM((r, gl), F32), pltpu.VMEM((r, li), F32),
        pltpu.VMEM((r, nl), F32),
        pltpu.VMEM((D, 8, li), jnp.int32),
        pltpu.VMEM((C, rl, li), BF), pltpu.VMEM((C, rl, li), BF),
        pltpu.VMEM((D, rl, li), BF), pltpu.VMEM((rl, gl), F32),
        pltpu.VMEM((C, rl, gl), BF),
        pltpu.VMEM((C, rl, gc), BF), pltpu.VMEM((C, rl, gc), BF),
        pltpu.VMEM((D, rl, li), BF), pltpu.VMEM((D, rl, li), BF),
        pltpu.VMEM((C, rl, li), BF),
        pltpu.VMEM((C, r, nl), BF),
        pltpu.VMEM((D, span, rl, gc), BF), pltpu.VMEM((D, span, rl, gc), BF),
        pltpu.VMEM((r, nl), BF),
        pltpu.SemaphoreType.DMA((CHUNKS + 2,)),
        pltpu.SemaphoreType.DMA((10, C)), pltpu.SemaphoreType.DMA((10, C)),
        pltpu.SemaphoreType.DMA((CHUNKS, C)), pltpu.SemaphoreType.DMA((CHUNKS, C)),
    ]
    out, sol = pl.pallas_call(
        functools.partial(kernel, C, D),
        out_shape=(jax.ShapeDtypeStruct((r, nl), BF), jax.ShapeDtypeStruct((rl, gc * C), BF)),
        in_specs=[pl.BlockSpec(memory_space=pltpu.SMEM), vmem, vmem, hbm, hbm, hbm],
        out_specs=(vmem, vmem),
        scratch_shapes=scratch,
        compiler_params=pltpu.CompilerParams(
            collective_id=0, has_side_effects=True, vmem_limit_bytes=60 * 1024 * 1024),
    )(block_ids, rhs_interior[0], rhs_interface, interior_inv[0], coupling[0], interface_inv)
    return out[None], sol


def solution(mesh):
    placed = (
        P("dom", "col", None),
        P("dom", None, "col"),
        P("dom", "col", None),
        P("col", "dom"),
        P("dom", None),
        P("dom", "col"),
    )
    return jax.shard_map(
        functools.partial(per_device, mesh.shape["col"], mesh.shape["dom"]),
        mesh=mesh,
        in_specs=placed,
        out_specs=(P("dom", None, "col"), P("col", None)),
        check_vma=False,
    )
```

```python
import functools

import jax
import jax.numpy as jnp
from jax import lax
from jax.experimental import pallas as pl
from jax.experimental.pallas import tpu as pltpu
from jax.sharding import PartitionSpec as P

BF = jnp.bfloat16
F32 = jnp.float32
MESH = pl.DeviceIdType.MESH
LANES = 128
CHUNKS = 8
HALVES = 2


def partner(me, o, n):
    total, bit = 0, 1
    while bit < n:
        total = total + lax.rem(lax.div(me, bit) + (o // bit) % 2, 2) * bit
        bit *= 2
    return total


def kernel(C, D, ids_ref, rhs_ref, ri_ref, inv_hbm, cp_hbm, ii_hbm, out_ref, sol_ref,
           inv, cp, ii, gath, xf, xg, xl, rhsl, idsb, s2, r2, g3, acc3, g4, s5, r5,
           s6, r6, g7, x8, r9, g10, stepb,
           ld, ss, rs, s1sem, r1sem, s8sem, r8sem):
    c = lax.axis_index("col")
    d = lax.axis_index("dom")
    rl, ni = rhs_ref.shape
    nl = inv.shape[1]
    li = cp.shape[1]
    gl = ii.shape[0]
    gc = ii.shape[1]
    kb = li // LANES
    w = ni // CHUNKS

    loads = []
    for j in range(CHUNKS):
        rows = pl.ds(j * w, w)
        loads.append(pltpu.make_async_copy(inv_hbm.at[rows, :], inv.at[rows, :], ld.at[j]))
    loads.append(pltpu.make_async_copy(cp_hbm, cp, ld.at[CHUNKS]))
    loads.append(pltpu.make_async_copy(ii_hbm, ii, ld.at[CHUNKS + 1]))
    for copy in loads:
        copy.start()

    barrier = pltpu.get_barrier_semaphore()
    for o in range(1, C):
        pl.semaphore_signal(barrier, inc=1, device_id={"col": partner(c, o, C)}, device_id_type=MESH)
    for o in range(1, D):
        pl.semaphore_signal(barrier, inc=1, device_id={"dom": partner(d, o, D)}, device_id_type=MESH)
    pl.semaphore_wait(barrier, C - 1 + D - 1)

    def send(src, dst, phase, o, axis, target):
        copy = pltpu.make_async_remote_copy(
            src_ref=src, dst_ref=dst, send_sem=ss.at[phase, o], recv_sem=rs.at[phase, o],
            device_id={axis: target}, device_id_type=MESH)
        copy.start()
        return copy

    done = []

    def part1(src, j, q, o, target):
        cols = pl.ds(j * w, w)
        copy = pltpu.make_async_remote_copy(
            src_ref=src.at[:, cols], dst_ref=gath.at[q, :, cols],
            send_sem=s1sem.at[j, o], recv_sem=r1sem.at[j, o],
            device_id={"col": target}, device_id_type=MESH)
        copy.start()
        done.append(copy)
        return copy

    far, near = [], []
    for j in range(CHUNKS):
        far.append([part1(rhs_ref, j, c, o, partner(c, o, C)) for o in reversed(range(2, C, 2))])
        near.append([part1(rhs_ref, j, c, 1, partner(c, 1, C))])
    gath[c] = rhs_ref[...]
    for k in range(kb):
        idsb[d, :, k * LANES:(k + 1) * LANES] = jnp.full((8, LANES), ids_ref[0, k], jnp.int32)
    idcopies = [send(idsb.at[d], idsb.at[d], 0, o, "dom", partner(d, o, D)) for o in range(1, D)]
    done += idcopies

    def dot1(j, acc):
        for copy in near[j]:
            copy.wait_recv()
        for q in range(C):
            xf[q * rl:(q + 1) * rl, :] = gath[q, :, j * w:(j + 1) * w].astype(F32)
        loads[j].wait()
        part = jnp.dot(xf[...].astype(BF), inv[j * w:(j + 1) * w, :], preferred_element_type=F32)
        return part if acc is None else acc + part

    acc = None
    for j in range(CHUNKS):
        for copy, o in zip(far[j], reversed(range(2, C, 2))):
            copy.wait_recv()
            q = partner(c, o, C)
            near[j].append(part1(gath.at[q], j, q, o + 1, partner(c, 1, C)))
        if j > 0:
            acc = dot1(j - 1, acc)
    acc = dot1(CHUNKS - 1, acc)
    stepb[...] = acc.astype(BF)

    loads[CHUNKS].wait()
    con = jnp.dot(stepb[...], cp[...], preferred_element_type=F32)
    for q in range(C):
        s2[q] = con[q * rl:(q + 1) * rl, :].astype(BF)
    copies = []
    for o in range(1, C):
        t = partner(c, o, C)
        copies.append(send(s2.at[t], r2.at[c], 1, o, "col", t))
    done += copies
    r2[c] = s2[c]
    for q in range(C):
        rhsl[q * rl:(q + 1) * rl, :] = gath[q, :, pl.ds(pl.multiple_of(c * nl, LANES), nl)].astype(F32)
    for copy in copies:
        copy.wait_recv()
    total = r2[0].astype(F32)
    for q in range(1, C):
        total = total + r2[q].astype(F32)

    g3[d] = total.astype(BF)
    copies = [send(g3.at[d], g3.at[d], 2, o, "dom", partner(d, o, D)) for o in range(1, D)]
    done += copies
    acc3[...] = ri_ref[...].astype(F32)
    for copy in idcopies:
        copy.wait_recv()
    for copy in copies:
        copy.wait_recv()
    base = d * (gl // LANES)

    def place(s, carry):
        ids = [idsb[s, 0:rl, k * LANES:(k + 1) * LANES] - base for k in range(kb)]
        val = [g3[s, :, k * LANES:(k + 1) * LANES].astype(F32) for k in range(kb)]
        for j in range(gl // LANES):
            part = jnp.zeros((rl, LANES), F32)
            for k in range(kb):
                part = jnp.where(ids[k] == j, val[k], part)
            at = slice(j * LANES, (j + 1) * LANES)
            acc3[:, at] = acc3[:, at] - part
        return carry

    lax.fori_loop(0, D, place, 0)

    g4[c] = acc3[...].astype(BF)
    copies = [send(g4.at[c], g4.at[c], 3, o, "col", partner(c, o, C)) for o in range(1, C)]
    done += copies
    loads[CHUNKS + 1].wait()
    for copy in copies:
        copy.wait_recv()
    for q in range(C):
        xg[q * rl:(q + 1) * rl, :] = g4[q].astype(F32)
    part = jnp.dot(xg[...].astype(BF), ii[...], preferred_element_type=F32)

    for q in range(C):
        s5[q] = part[q * rl:(q + 1) * rl, :].astype(BF)
    copies = []
    for o in range(1, C):
        t = partner(c, o, C)
        copies.append(send(s5.at[t], r5.at[c], 4, o, "col", t))
    done += copies
    r5[c] = s5[c]
    for copy in copies:
        copy.wait_recv()

    per = gc // LANES

    def pick(s, carry):
        ids = [idsb[s, 0:rl, k * LANES:(k + 1) * LANES] for k in range(kb)]
        got = [jnp.zeros((rl, LANES), F32) for k in range(kb)]
        for q in range(C):
            for j in range(per):
                block = r5[q, :, j * LANES:(j + 1) * LANES].astype(F32)
                got = [jnp.where(ids[k] == q * per + j, block, got[k]) for k in range(kb)]
        for k in range(kb):
            s6[s, :, k * LANES:(k + 1) * LANES] = got[k].astype(BF)
        return carry

    lax.fori_loop(0, D, pick, 0)
    copies = []
    for o in range(1, D):
        t = partner(d, o, D)
        copies.append(send(s6.at[t], r6.at[d], 5, o, "dom", t))
    done += copies
    span = C // D
    ninth = []
    for o in range(1, D):
        t = partner(d, o, D)
        ninth.append(send(r5.at[pl.ds(t * span, span)], r9.at[d], 6, o, "dom", t))
    done += ninth
    r6[d] = s6[d]
    for q in range(span):
        r9[d, q] = r5[d * span + q]
    for copy in copies:
        copy.wait_recv()
    total = r6[0].astype(F32)
    for s in range(1, D):
        total = total + r6[s].astype(F32)

    g7[c] = total.astype(BF)
    copies = [send(g7.at[c], g7.at[c], 7, o, "col", partner(c, o, C)) for o in range(1, C)]
    done += copies
    for copy in copies:
        copy.wait_recv()
    for q in range(C):
        xl[q * rl:(q + 1) * rl, :] = g7[q].astype(F32)
    corr = lax.dot_general(xl[...].astype(BF), cp[...], (((1,), (1,)), ((), ())), preferred_element_type=F32)

    x8[c] = (rhsl[...] - corr).astype(BF)
    wide = nl // HALVES

    def part8(h, q, o, target):
        cols = pl.ds(h * wide, wide)
        copy = pltpu.make_async_remote_copy(
            src_ref=x8.at[q, :, cols], dst_ref=x8.at[q, :, cols],
            send_sem=s8sem.at[h, o], recv_sem=r8sem.at[h, o],
            device_id={"col": target}, device_id_type=MESH)
        copy.start()
        done.append(copy)
        return copy

    far, near = [], []
    for h in range(HALVES):
        far.append([part8(h, c, o, partner(c, o, C)) for o in reversed(range(2, C, 2))])
    side = [part8(h, c, 1, partner(c, 1, C)) for h in range(HALVES)]

    for copy in ninth:
        copy.wait_recv()
    for q in range(span):
        total = r9[0, q].astype(F32)
        for s in range(1, D):
            total = total + r9[s, q].astype(F32)
        g10[d, q] = total.astype(BF)
    tenth = [send(g10.at[d], g10.at[d], 9, o, "dom", partner(d, o, D)) for o in range(1, D)]
    done += tenth

    def dot8(h, o):
        q = partner(c, o, C)
        rows = pl.ds(pl.multiple_of(q * nl + h * wide, LANES), wide)
        return jnp.dot(x8[q, :, h * wide:(h + 1) * wide], inv[rows, :], preferred_element_type=F32)

    acc = dot8(0, 0)
    for h in range(1, HALVES):
        acc = acc + dot8(h, 0)
    for h in range(HALVES):
        side[h].wait_recv()
        acc = acc + dot8(h, 1)
    order = list(reversed(range(2, C, 2)))
    for h in range(HALVES):
        for copy, o in zip(far[h], order):
            copy.wait_recv()
            near.append(part8(h, partner(c, o, C), o + 1, partner(c, 1, C)))
            acc = acc + dot8(h, o)
    for h in range(HALVES):
        for i, o in enumerate(order):
            near[h * len(order) + i].wait_recv()
            acc = acc + dot8(h, o + 1)
    out_ref[...] = acc.astype(BF)

    for copy in tenth:
        copy.wait_recv()
    for s in range(D):
        for q in range(span):
            at = (s * span + q) * gc
            sol_ref[:, at:at + gc] = g10[s, q]
    for copy in done:
        copy.wait_send()


def per_device(C, D, rhs_interior, interior_inv, coupling, rhs_interface, block_ids, interface_inv):
    rl, ni = rhs_interior.shape[1:]
    nl = interior_inv.shape[2]
    li = coupling.shape[2]
    gl, gc = interface_inv.shape
    r = rl * C
    span = C // D
    vmem = pl.BlockSpec(memory_space=pltpu.VMEM)
    hbm = pl.BlockSpec(memory_space=pl.ANY)
    scratch = [
        pltpu.VMEM((ni, nl), BF), pltpu.VMEM((coupling.shape[1], li), BF), pltpu.VMEM((gl, gc), BF),
        pltpu.VMEM((C, rl, ni), BF),
        pltpu.VMEM((r, ni // CHUNKS), F32), pltpu.VMEM((r, gl), F32), pltpu.VMEM((r, li), F32),
        pltpu.VMEM((r, nl), F32),
        pltpu.VMEM((D, 8, li), jnp.int32),
        pltpu.VMEM((C, rl, li), BF), pltpu.VMEM((C, rl, li), BF),
        pltpu.VMEM((D, rl, li), BF), pltpu.VMEM((rl, gl), F32),
        pltpu.VMEM((C, rl, gl), BF),
        pltpu.VMEM((C, rl, gc), BF), pltpu.VMEM((C, rl, gc), BF),
        pltpu.VMEM((D, rl, li), BF), pltpu.VMEM((D, rl, li), BF),
        pltpu.VMEM((C, rl, li), BF),
        pltpu.VMEM((C, r, nl), BF),
        pltpu.VMEM((D, span, rl, gc), BF), pltpu.VMEM((D, span, rl, gc), BF),
        pltpu.VMEM((r, nl), BF),
        pltpu.SemaphoreType.DMA((CHUNKS + 2,)),
        pltpu.SemaphoreType.DMA((10, C)), pltpu.SemaphoreType.DMA((10, C)),
        pltpu.SemaphoreType.DMA((CHUNKS, C)), pltpu.SemaphoreType.DMA((CHUNKS, C)),
        pltpu.SemaphoreType.DMA((HALVES, C)), pltpu.SemaphoreType.DMA((HALVES, C)),
    ]
    out, sol = pl.pallas_call(
        functools.partial(kernel, C, D),
        out_shape=(jax.ShapeDtypeStruct((r, nl), BF), jax.ShapeDtypeStruct((rl, gc * C), BF)),
        in_specs=[pl.BlockSpec(memory_space=pltpu.SMEM), vmem, vmem, hbm, hbm, hbm],
        out_specs=(vmem, vmem),
        scratch_shapes=scratch,
        compiler_params=pltpu.CompilerParams(
            collective_id=0, has_side_effects=True, vmem_limit_bytes=60 * 1024 * 1024),
    )(block_ids, rhs_interior[0], rhs_interface, interior_inv[0], coupling[0], interface_inv)
    return out[None], sol


def solution(mesh):
    placed = (
        P("dom", "col", None),
        P("dom", None, "col"),
        P("dom", "col", None),
        P("col", "dom"),
        P("dom", None),
        P("dom", "col"),
    )
    return jax.shard_map(
        functools.partial(per_device, mesh.shape["col"], mesh.shape["dom"]),
        mesh=mesh,
        in_specs=placed,
        out_specs=(P("dom", None, "col"), P("col", None)),
        check_vma=False,
    )
```

```python
import functools

import jax
import jax.numpy as jnp
from jax import lax
from jax.experimental import pallas as pl
from jax.experimental.pallas import tpu as pltpu
from jax.sharding import PartitionSpec as P

BF = jnp.bfloat16
F32 = jnp.float32
MESH = pl.DeviceIdType.MESH
LANES = 128
CHUNKS = 8
HALVES = 2


def partner(me, o, n):
    total, bit = 0, 1
    while bit < n:
        total = total + lax.rem(lax.div(me, bit) + (o // bit) % 2, 2) * bit
        bit *= 2
    return total


def kernel(C, D, ids_hbm, rhs_hbm, ri_hbm, inv_hbm, cp_hbm, ii_hbm, out_hbm, sol_hbm,
           ids_ref, ri_ref, outb, inv, cp, ii, gath, xf, xg, xl, rhsl, idsb, s2, r2, g3, acc3, g4, s5, r5,
           f6, s6, r6, g7, x8, r9, g10, stepb,
           ld, st, ss, rs, s1sem, r1sem, s8sem, r8sem):
    c = lax.axis_index("col")
    d = lax.axis_index("dom")
    rl, ni = rhs_hbm.shape
    nl = inv.shape[1]
    li = cp.shape[1]
    gl = ii.shape[0]
    gc = ii.shape[1]
    kb = li // LANES
    w = ni // CHUNKS

    rhs_load = pltpu.make_async_copy(rhs_hbm, gath.at[c], ld.at[CHUNKS + 2])
    ids_load = pltpu.make_async_copy(ids_hbm, ids_ref, ld.at[CHUNKS + 3])
    ri_load = pltpu.make_async_copy(ri_hbm, ri_ref, ld.at[CHUNKS + 4])
    rhs_load.start()
    ids_load.start()
    ri_load.start()
    loads = []
    for j in range(CHUNKS):
        rows = pl.ds(j * w, w)
        loads.append(pltpu.make_async_copy(inv_hbm.at[rows, :], inv.at[rows, :], ld.at[j]))
    loads.append(pltpu.make_async_copy(cp_hbm, cp, ld.at[CHUNKS]))
    loads.append(pltpu.make_async_copy(ii_hbm, ii, ld.at[CHUNKS + 1]))
    for copy in loads:
        copy.start()

    barrier = pltpu.get_barrier_semaphore()
    for o in range(1, C):
        pl.semaphore_signal(barrier, inc=1, device_id={"col": partner(c, o, C)}, device_id_type=MESH)
    for o in range(1, D):
        pl.semaphore_signal(barrier, inc=1, device_id={"dom": partner(d, o, D)}, device_id_type=MESH)
    pl.semaphore_wait(barrier, C - 1 + D - 1)

    def send(src, dst, phase, o, axis, target):
        copy = pltpu.make_async_remote_copy(
            src_ref=src, dst_ref=dst, send_sem=ss.at[phase, o], recv_sem=rs.at[phase, o],
            device_id={axis: target}, device_id_type=MESH)
        copy.start()
        return copy

    done = []

    def part1(src, j, q, o, target):
        cols = pl.ds(j * w, w)
        copy = pltpu.make_async_remote_copy(
            src_ref=src.at[:, cols], dst_ref=gath.at[q, :, cols],
            send_sem=s1sem.at[j, o], recv_sem=r1sem.at[j, o],
            device_id={"col": target}, device_id_type=MESH)
        copy.start()
        done.append(copy)
        return copy

    rhs_load.wait()
    far, near = [], []
    for j in range(CHUNKS):
        far.append([part1(gath.at[c], j, c, o, partner(c, o, C)) for o in reversed(range(2, C, 2))])
        near.append([part1(gath.at[c], j, c, 1, partner(c, 1, C))])
    ids_load.wait()
    for k in range(kb):
        idsb[d, :, k * LANES:(k + 1) * LANES] = jnp.full((8, LANES), ids_ref[0, k], jnp.int32)
    idcopies = [send(idsb.at[d], idsb.at[d], 0, o, "dom", partner(d, o, D)) for o in reversed(range(1, D))]
    done += idcopies

    def dot1(j, acc):
        for copy in near[j]:
            copy.wait_recv()
        for q in range(C):
            xf[q * rl:(q + 1) * rl, :] = gath[q, :, j * w:(j + 1) * w].astype(F32)
        loads[j].wait()
        part = jnp.dot(xf[...].astype(BF), inv[j * w:(j + 1) * w, :], preferred_element_type=F32)
        return part if acc is None else acc + part

    acc = None
    for j in range(CHUNKS):
        for copy, o in zip(far[j], reversed(range(2, C, 2))):
            copy.wait_recv()
            q = partner(c, o, C)
            near[j].append(part1(gath.at[q], j, q, o + 1, partner(c, 1, C)))
        if j > 0:
            acc = dot1(j - 1, acc)
    acc = dot1(CHUNKS - 1, acc)
    stepb[...] = acc.astype(BF)

    loads[CHUNKS].wait()
    con = jnp.dot(stepb[...], cp[...], preferred_element_type=F32)
    for q in range(C):
        s2[q] = con[q * rl:(q + 1) * rl, :].astype(BF)
    copies = []
    for o in reversed(range(1, C)):
        t = partner(c, o, C)
        copies.append(send(s2.at[t], r2.at[c], 1, o, "col", t))
    done += copies
    r2[c] = s2[c]
    for q in range(C):
        rhsl[q * rl:(q + 1) * rl, :] = gath[q, :, pl.ds(pl.multiple_of(c * nl, LANES), nl)].astype(F32)
    for copy in copies:
        copy.wait_recv()
    total = r2[0].astype(F32)
    for q in range(1, C):
        total = total + r2[q].astype(F32)

    g3[d] = total.astype(BF)
    copies = [send(g3.at[d], g3.at[d], 2, o, "dom", partner(d, o, D)) for o in reversed(range(1, D))]
    done += copies
    ri_load.wait()
    acc3[...] = ri_ref[...].astype(F32)
    for copy in idcopies:
        copy.wait_recv()
    for copy in copies:
        copy.wait_recv()
    base = d * (gl // LANES)

    def place(s, carry):
        ids = [idsb[s, 0:rl, k * LANES:(k + 1) * LANES] - base for k in range(kb)]
        val = [g3[s, :, k * LANES:(k + 1) * LANES].astype(F32) for k in range(kb)]
        for j in range(gl // LANES):
            part = jnp.zeros((rl, LANES), F32)
            for k in range(kb):
                part = jnp.where(ids[k] == j, val[k], part)
            at = slice(j * LANES, (j + 1) * LANES)
            acc3[:, at] = acc3[:, at] - part
        return carry

    lax.fori_loop(0, D, place, 0)

    g4[c] = acc3[...].astype(BF)
    half = gl // 2
    sides = []
    for h in range(2):
        cols = pl.ds(h * half, half)
        sides.append([send(g4.at[c, :, cols], g4.at[c, :, cols], 3 + 7 * h, o, "col", partner(c, o, C))
                      for o in reversed(range(1, C))])
        done += sides[h]
    loads[CHUNKS + 1].wait()
    part = None
    for h in range(2):
        for copy in sides[h]:
            copy.wait_recv()
        for q in range(C):
            xg[q * rl:(q + 1) * rl, :] = g4[q, :, h * half:(h + 1) * half].astype(F32)
        piece = jnp.dot(xg[...].astype(BF), ii[h * half:(h + 1) * half, :], preferred_element_type=F32)
        part = piece if part is None else part + piece

    for q in range(C):
        s5[q] = part[q * rl:(q + 1) * rl, :].astype(BF)
    copies = []
    for o in reversed(range(1, C)):
        t = partner(c, o, C)
        copies.append(send(s5.at[t], r5.at[c], 4, o, "col", t))
    done += copies
    r5[c] = s5[c]

    per = gc // LANES
    for o in range(C):
        if o > 0:
            copies[C - 1 - o].wait_recv()
        q = partner(c, o, C)

        def pick(s, carry):
            blocks = [r5[q, :, j * LANES:(j + 1) * LANES].astype(F32) for j in range(per)]
            for k in range(kb):
                at = slice(k * LANES, (k + 1) * LANES)
                ids = idsb[s, 0:rl, at] - q * per
                got = jnp.zeros((rl, LANES), F32) if o == 0 else f6[s, :, at]
                for j in range(per):
                    got = jnp.where(ids == j, blocks[j], got)
                f6[s, :, at] = got
            return carry

        lax.fori_loop(0, D, pick, 0)
    for s in range(D):
        s6[s] = f6[s].astype(BF)
    copies = []
    for o in reversed(range(1, D)):
        t = partner(d, o, D)
        copies.append(send(s6.at[t], r6.at[d], 5, o, "dom", t))
    done += copies
    span = C // D
    ninth = []
    for o in reversed(range(1, D)):
        t = partner(d, o, D)
        ninth.append(send(r5.at[pl.ds(t * span, span)], r9.at[d], 6, o, "dom", t))
    done += ninth
    r6[d] = s6[d]
    for q in range(span):
        r9[d, q] = r5[d * span + q]
    for copy in copies:
        copy.wait_recv()
    total = r6[0].astype(F32)
    for s in range(1, D):
        total = total + r6[s].astype(F32)

    g7[c] = total.astype(BF)
    copies = [send(g7.at[c], g7.at[c], 7, o, "col", partner(c, o, C)) for o in reversed(range(1, C))]
    done += copies
    for copy in copies:
        copy.wait_recv()
    for q in range(C):
        xl[q * rl:(q + 1) * rl, :] = g7[q].astype(F32)
    corr = lax.dot_general(xl[...].astype(BF), cp[...], (((1,), (1,)), ((), ())), preferred_element_type=F32)

    x8[c] = (rhsl[...] - corr).astype(BF)
    wide = nl // HALVES

    def part8(h, q, o, target):
        cols = pl.ds(h * wide, wide)
        copy = pltpu.make_async_remote_copy(
            src_ref=x8.at[q, :, cols], dst_ref=x8.at[q, :, cols],
            send_sem=s8sem.at[h, o], recv_sem=r8sem.at[h, o],
            device_id={"col": target}, device_id_type=MESH)
        copy.start()
        done.append(copy)
        return copy

    far, near = [], []
    for h in range(HALVES):
        far.append([part8(h, c, o, partner(c, o, C)) for o in reversed(range(2, C, 2))])
    side = [part8(h, c, 1, partner(c, 1, C)) for h in range(HALVES)]

    for copy in ninth:
        copy.wait_recv()
    for q in range(span):
        total = r9[0, q].astype(F32)
        for s in range(1, D):
            total = total + r9[s, q].astype(F32)
        g10[d, q] = total.astype(BF)
    tenth = [send(g10.at[d], g10.at[d], 9, o, "dom", partner(d, o, D)) for o in reversed(range(1, D))]
    done += tenth

    def dot8(h, o):
        q = partner(c, o, C)
        rows = pl.ds(pl.multiple_of(q * nl + h * wide, LANES), wide)
        return jnp.dot(x8[q, :, h * wide:(h + 1) * wide], inv[rows, :], preferred_element_type=F32)

    acc = dot8(0, 0)
    for h in range(1, HALVES):
        acc = acc + dot8(h, 0)
    for h in range(HALVES):
        side[h].wait_recv()
        acc = acc + dot8(h, 1)
    order = list(reversed(range(2, C, 2)))
    for h in range(HALVES):
        for copy, o in zip(far[h], order):
            copy.wait_recv()
            near.append(part8(h, partner(c, o, C), o + 1, partner(c, 1, C)))
            acc = acc + dot8(h, o)
    stores = []
    for copy in tenth:
        copy.wait_recv()
    for s in range(D):
        for q in range(span):
            n = s * span + q
            store = pltpu.make_async_copy(g10.at[s, q], sol_hbm.at[:, pl.ds(n * gc, gc)], st.at[n])
            store.start()
            stores.append(store)
    for h in range(HALVES):
        for i, o in enumerate(order):
            near[h * len(order) + i].wait_recv()
            acc = acc + dot8(h, o + 1)
    outb[...] = acc.astype(BF)
    stores.append(pltpu.make_async_copy(outb, out_hbm, st.at[C]))
    stores[-1].start()

    for store in stores:
        store.wait()
    for copy in done:
        copy.wait_send()


def keep(a_hbm, b_hbm, a_out, b_out, a_buf, b_buf, sem):
    first = [pltpu.make_async_copy(a_hbm, a_buf, sem.at[0]), pltpu.make_async_copy(b_hbm, b_buf, sem.at[1])]
    then = [pltpu.make_async_copy(a_buf, a_out, sem.at[2]), pltpu.make_async_copy(b_buf, b_out, sem.at[3])]
    for copy in first:
        copy.start()
    for copy, after in zip(first, then):
        copy.wait()
        after.start()
    for copy in then:
        copy.wait()


def per_device(C, D, rhs_interior, interior_inv, coupling, rhs_interface, block_ids, interface_inv):
    rl, ni = rhs_interior.shape[1:]
    nl = interior_inv.shape[2]
    li = coupling.shape[2]
    gl, gc = interface_inv.shape
    r = rl * C
    span = C // D
    ids_shape = block_ids.shape
    hbm = pl.BlockSpec(memory_space=pl.ANY)
    scratch = [
        pltpu.SMEM(ids_shape, jnp.int32), pltpu.VMEM((rl, gl), BF), pltpu.VMEM((r, nl), BF),
        pltpu.VMEM((ni, nl), BF), pltpu.VMEM((coupling.shape[1], li), BF), pltpu.VMEM((gl, gc), BF),
        pltpu.VMEM((C, rl, ni), BF),
        pltpu.VMEM((r, ni // CHUNKS), F32), pltpu.VMEM((r, gl // 2), F32), pltpu.VMEM((r, li), F32),
        pltpu.VMEM((r, nl), F32),
        pltpu.VMEM((D, 8, li), jnp.int32),
        pltpu.VMEM((C, rl, li), BF), pltpu.VMEM((C, rl, li), BF),
        pltpu.VMEM((D, rl, li), BF), pltpu.VMEM((rl, gl), F32),
        pltpu.VMEM((C, rl, gl), BF),
        pltpu.VMEM((C, rl, gc), BF), pltpu.VMEM((C, rl, gc), BF),
        pltpu.VMEM((D, rl, li), F32),
        pltpu.VMEM((D, rl, li), BF), pltpu.VMEM((D, rl, li), BF),
        pltpu.VMEM((C, rl, li), BF),
        pltpu.VMEM((C, r, nl), BF),
        pltpu.VMEM((D, span, rl, gc), BF), pltpu.VMEM((D, span, rl, gc), BF),
        pltpu.VMEM((r, nl), BF),
        pltpu.SemaphoreType.DMA((CHUNKS + 5,)), pltpu.SemaphoreType.DMA((C + 1,)),
        pltpu.SemaphoreType.DMA((11, C)), pltpu.SemaphoreType.DMA((11, C)),
        pltpu.SemaphoreType.DMA((CHUNKS, C)), pltpu.SemaphoreType.DMA((CHUNKS, C)),
        pltpu.SemaphoreType.DMA((HALVES, C)), pltpu.SemaphoreType.DMA((HALVES, C)),
    ]
    out, sol = pl.pallas_call(
        functools.partial(kernel, C, D),
        out_shape=(jax.ShapeDtypeStruct((r, nl), BF), jax.ShapeDtypeStruct((rl, gc * C), BF)),
        in_specs=[hbm] * 6,
        out_specs=(hbm, hbm),
        scratch_shapes=scratch,
        compiler_params=pltpu.CompilerParams(
            collective_id=0, has_side_effects=True, vmem_limit_bytes=60 * 1024 * 1024),
    )(block_ids, rhs_interior[0], rhs_interface, interior_inv[0], coupling[0], interface_inv)
    out, sol = pl.pallas_call(
        keep,
        out_shape=(jax.ShapeDtypeStruct(out.shape, BF), jax.ShapeDtypeStruct(sol.shape, BF)),
        in_specs=[hbm, hbm],
        out_specs=(hbm, hbm),
        scratch_shapes=[pltpu.VMEM(out.shape, BF), pltpu.VMEM(sol.shape, BF), pltpu.SemaphoreType.DMA((4,))],
    )(out, sol)
    return out[None], sol


def solution(mesh):
    placed = (
        P("dom", "col", None),
        P("dom", None, "col"),
        P("dom", "col", None),
        P("col", "dom"),
        P("dom", None),
        P("dom", "col"),
    )
    return jax.shard_map(
        functools.partial(per_device, mesh.shape["col"], mesh.shape["dom"]),
        mesh=mesh,
        in_specs=placed,
        out_specs=(P("dom", None, "col"), P("col", None)),
        check_vma=False,
    )
```
